256 devices in a mesh: row: 32 (over x_lo, z, core), col: 8 (over x_hi, y).
Axes of the slice: x: 4 (x_hi: 2, x_lo: 2; x = x_hi * 2 + x_lo), y: 4, z: 8, core: 2. Of those that a mesh axis runs over, the one named last changes fastest.
Arguments:
- joined: bfloat16 [2, 32, 32, 28, 4096], P(None, None, 'row', None, 'col'), may hold values from -0.09375 to 0.09375
- probes: bfloat16 [2, 128, 4096], P(None, None, 'col'), may hold values from -6 to 6
Outputs:
- gate_rows: bfloat16 [2, 14336, 4096], P(None, 'row', 'col')
- up_rows: bfloat16 [2, 14336, 4096], P(None, 'row', 'col')
- hidden: bfloat16 [2, 128, 14336], P(None, 'col', 'row')
The draws below stay inside these ranges and needn't reach their ends.
All inputs are finite; a program needn't handle non-finite values.
Results may differ from the reference program's by a relative error of at most 0.002.
Values may be sent and summed in bfloat16 or wider, within the bound.
No kernel may reach another device: no remote copies, remote signals or barrier semaphores. Data moves between devices by JAX's collectives and lax.ppermute only.
A program may use at most 64 MiB of HBM per device.

```python
import jax
import jax.numpy as jnp

D = 4096
FF = 14336
HALF = 14
LAYERS = 2
TOKENS = 128
CYCLES = 32
N_ROW = 32


def block_levels(rng, dims, split, least, largest):
    factor_of = 1.0
    for dim, blocks in split:
        heights = jax.random.uniform(jax.random.fold_in(jax.random.fold_in(rng, 6), dim), (blocks,), jnp.float32, least / len(split), largest / len(split))
        factor_of = factor_of * jnp.repeat(jnp.exp(heights), dims[dim] // blocks).reshape((-1,) + (1,) * (len(dims) - 1 - dim))
    return factor_of


def gaussian(rng, extent, deviation, reach, split=(), held_as=jnp.bfloat16):
    values = deviation * jax.random.normal(rng, extent, jnp.float32)
    if split:
        values = values * block_levels(rng, extent, split, -0.22, 0.18)
    return jnp.clip(values, -reach, reach).astype(held_as)


def setup_inputs(seed: int = 0) -> dict:
    splits = jax.random.split(jax.random.key(seed), 3)
    return {
        "joined": gaussian(splits[0], (LAYERS, CYCLES, N_ROW, 2 * HALF, D), D ** -0.5, 0.09375, ((2, 32), (4, 8))),
        "probes": gaussian(splits[1], (LAYERS, TOKENS, D), 1.0, 6.0, ((2, 8),)),
    }


def reference(joined, probes):
    blocks = joined.reshape(LAYERS, CYCLES * N_ROW, HALF, 2, D)
    gate_rows = blocks[:, :, :, 0, :].reshape(LAYERS, FF, D)
    up_rows = blocks[:, :, :, 1, :].reshape(LAYERS, FF, D)
    results = []
    for layer_index in range(LAYERS):
        gate_proj = jnp.dot(probes[layer_index], gate_rows[layer_index].T, preferred_element_type=jnp.float32)
        up_proj = jnp.dot(probes[layer_index], up_rows[layer_index].T, preferred_element_type=jnp.float32)
        results.append((jax.nn.silu(gate_proj) * up_proj).astype(jnp.bfloat16))
    hidden = jnp.stack(results, axis=0)
    return gate_rows, up_rows, hidden
```

```python
import jax
import jax.numpy as jnp
from jax import lax
from jax.experimental import pallas as pl
from jax.experimental.pallas import tpu as pltpu
from jax.sharding import Mesh
from jax.sharding import PartitionSpec as P

ROW = ("xlo", "z", "core")
COL = ("xhi", "y")
NX, NZ, NC = 2, 8, 2
EARLY = (3, 5)
LATE = (2, 6, 1, 7)
FLIPPED = (0,) + LATE
PIECES = tuple((a, s) for s in EARLY for a in (0, 1)) + ((0, 4), (1, 4)) + tuple((1, s) for s in FLIPPED) + tuple((0, s) for s in LATE) + ((0, 0),)
PIECE = (56, 512)


def row_index(x, z, c):
    return (x * NZ + z) * NC + c


def hop(a, s, b):
    return [
        (row_index(x, z, c), row_index(x ^ a, (z + s) % NZ, c ^ b))
        for x in range(NX)
        for z in range(NZ)
        for c in range(NC)
    ]


def vmem(*shape, dtype=jnp.bfloat16):
    return pltpu.VMEM(shape, dtype)


def hbm(*shape, dtype=jnp.bfloat16):
    return pltpu.HBM(shape, dtype)


def inside(x):
    return pltpu.with_memory_space_constraint(x, pltpu.VMEM)


def outside(x):
    return pltpu.with_memory_space_constraint(x, pltpu.HBM)


WHOLE = pl.BlockSpec(memory_space=pltpu.VMEM)
ANYWHERE = pl.BlockSpec(memory_space=pl.ANY)
INHBM = pl.BlockSpec(memory_space=pltpu.HBM)


def params(mib):
    return pltpu.CompilerParams(vmem_limit_bytes=mib << 20)


def selection(pieces, row_bits):
    x, z, c = lax.axis_index("xlo"), lax.axis_index("z"), lax.axis_index("core")
    row = lax.broadcasted_iota(jnp.int32, (16 * len(pieces), 256), 0)
    column = lax.broadcasted_iota(jnp.int32, (16 * len(pieces), 256), 1)
    j, b, n = row & 7, (row >> 3) & 1, row >> 4
    flip, step = jnp.zeros_like(n), jnp.zeros_like(n)
    for i, (a, s) in enumerate(pieces):
        flip = jnp.where(n == i, a, flip)
        step = jnp.where(n == i, s, step)
    block = ((flip ^ x) << 4) + (((z + step) & 7) << 1) + (b ^ c)
    return (column == (j << row_bits) + block).astype(jnp.bfloat16)


def pack_first_kernel(w_hbm, *refs):
    outs, w, sems = refs[:2], refs[2], refs[3]
    copies = [pltpu.make_async_copy(w_hbm.at[pl.ds(8 * g, 8)], w.at[pl.ds(8 * g, 8)], sems.at[g]) for g in range(7)]
    for copy in copies:
        copy.start()
    pick = selection(PIECES[:4], 5)
    for g in range(7):
        copies[g].wait()
        rows = w[8 * g : 8 * g + 8].reshape(256, 512)
        moved = jnp.dot(pick, rows, preferred_element_type=jnp.float32).astype(jnp.bfloat16)
        moved = moved.reshape(2, 2, 2, 8, 512)
        for i in range(2):
            outs[i][:, :, 8 * g : 8 * g + 8, :] = moved[i]


def pack_first(w):
    return pl.pallas_call(
        pack_first_kernel,
        out_shape=[vmem(2, 2, *PIECE)] * 2 + [vmem(56, 32, 512)],
        in_specs=[INHBM],
        out_specs=[WHOLE] * 3,
        scratch_shapes=[pltpu.SemaphoreType.DMA((7,))],
        compiler_params=params(4),
        name="pack_first",
    )(outside(w))


def pack_second_kernel(w, probes_hbm, *refs):
    outs, parts, (held, probes, proj, sems, out_sems, part_sems) = refs[:8], refs[8:12], refs[12:]
    y = lax.axis_index("y")
    first = pltpu.make_async_copy(probes_hbm, probes, sems.at[0])
    first.start()
    pick = selection(PIECES[4:], 5)
    dims = (((1,), (1,)), ((), ()))
    sent = []

    def ship(half, begin, count):
        rows = pl.ds(begin, count)
        pairs = [(held.at[i, :, rows], outs[i].at[:, rows]) for i in range(2)]
        pairs.append((held.at[pl.ds(2, 5), :, rows], outs[2].at[:, :, rows]))
        pairs += [(held.at[7 + i, :, rows], outs[3 + i].at[0, :, rows]) for i in range(4)]
        pairs.append((held.at[11, :, rows], outs[7].at[:, rows]))
        for i, (source, target) in enumerate(pairs):
            sent.append(pltpu.make_async_copy(source, target, out_sems.at[8 * half + i]))
            sent[-1].start()

    for layer in range(2):
        part = w[28 * layer : 28 * layer + 28].reshape(896, 512)
        if layer == 0:
            first.wait()
        product = lax.dot_general(probes[layer], part, dims, preferred_element_type=jnp.float32)
        proj[layer] = product.reshape(8, 16, 896)
        for s in range(1, 4):
            for h in range(2):
                n = len(sent)
                source = proj.at[layer, 4 * h + ((y + s) & 3)]
                sent.append(pltpu.make_async_copy(source, parts[s].at[h, layer], part_sems.at[n]))
                sent[-1].start()
        for h in range(2):
            parts[0][h, layer] = proj[layer, 4 * h + y]
    for g in range(7):
        rows = w[8 * g : 8 * g + 8].reshape(256, 512)
        moved = jnp.dot(pick, rows, preferred_element_type=jnp.float32).astype(jnp.bfloat16)
        held[:, :, 8 * g : 8 * g + 8, :] = moved.reshape(12, 2, 8, 512)
        if g == 3:
            ship(0, 0, 32)
    ship(1, 32, 24)
    for copy in sent:
        copy.wait()


def pack_second(w, probes):
    return pl.pallas_call(
        pack_second_kernel,
        out_shape=[hbm(2, *PIECE)] * 2
        + [hbm(5, 2, *PIECE)]
        + [hbm(2, 2, *PIECE)] * 4
        + [hbm(2, *PIECE)]
        + [vmem(2, 2, 16, 896, dtype=jnp.float32)]
        + [hbm(2, 2, 16, 896, dtype=jnp.float32)] * 3,
        in_specs=[WHOLE, INHBM],
        out_specs=[INHBM] * 8 + [WHOLE] + [INHBM] * 3,
        scratch_shapes=[
            pltpu.VMEM((12, 2, 56, 512), jnp.bfloat16),
            pltpu.VMEM((2, 128, 512), jnp.bfloat16),
            pltpu.VMEM((2, 8, 16, 896), jnp.float32),
            pltpu.SemaphoreType.DMA((1,)),
            pltpu.SemaphoreType.DMA((16,)),
            pltpu.SemaphoreType.DMA((12,)),
        ],
        compiler_params=params(8),
        name="pack_second",
    )(inside(w), outside(probes))


def join_kernel(crossed, *refs):
    outs, sems = refs[4:8], refs[8]
    copies = [pltpu.make_async_copy(crossed.at[1 + n], out.at[1], sems.at[n]) for n, out in enumerate(outs)]
    for copy in copies:
        copy.start()
    for copy in copies:
        copy.wait()


def join(crossed, straight):
    return pl.pallas_call(
        join_kernel,
        out_shape=[hbm(2, 2, *PIECE)] * 4,
        in_specs=[WHOLE] + [INHBM] * 4,
        out_specs=[INHBM] * 4,
        scratch_shapes=[pltpu.SemaphoreType.DMA((4,))],
        input_output_aliases={1: 0, 2: 1, 3: 2, 4: 3},
        compiler_params=params(1),
        name="join",
    )(inside(crossed), *map(outside, straight))


def gather_kernel(*refs):
    pieces, out, sems = refs[:2], refs[2], refs[3]
    copies = [pltpu.make_async_copy(piece.at[1], out.at[n], sems.at[n]) for n, piece in enumerate(pieces)]
    for copy in copies:
        copy.start()
    for copy in copies:
        copy.wait()


def gather(pieces):
    return pl.pallas_call(
        gather_kernel,
        out_shape=vmem(2, 2, *PIECE),
        in_specs=[ANYWHERE] * 2,
        out_specs=WHOLE,
        scratch_shapes=[pltpu.SemaphoreType.DMA((2,))],
        compiler_params=params(1),
        name="gather",
    )(*pieces)


def unpack_kernel(*refs):
    early, late, (gate_hbm, up_hbm, held, rows_out, sems, out_sems) = refs[:14], refs[14:22], refs[22:]
    x, z, c = lax.axis_index("xlo"), lax.axis_index("z"), lax.axis_index("core")
    local, crossed, z3, z5, d04, d14, post = early[0:2], early[2:4], early[4:6], early[6:8], early[8:10], early[10:12], early[12:14]
    pieces = []
    for b in range(2):
        pieces += [(local[b].at[b], 0, 0, b), (crossed[b].at[0, b], 1, 0, b)]
        pieces += [(z3[b].at[0, b], 0, 3, b), (post[b].at[0, b], 1, 3, b)]
        pieces += [(z5[b].at[0, b], 0, 5, b), (post[b].at[1, b], 1, 5, b)]
        pieces += [(d04[b].at[b], 0, 4, b), (d14[b].at[b], 1, 4, b)]

    def place(a, s, b):
        return (a ^ x) * 4 + (((z - s) & 7) >> 1), (z - s) & 1, b ^ c

    copies = []
    for source, a, s, b in pieces:
        copies.append(pltpu.make_async_copy(source, held.at[place(a, s, b)], sems.at[len(copies)]))
        copies[-1].start()
    out = lax.broadcasted_iota(jnp.int32, (224, 224), 0)
    inn = lax.broadcasted_iota(jnp.int32, (224, 224), 1)
    source = jnp.zeros((224, 224), jnp.int32)
    for q in range(4):
        for layer in range(2):
            for g in range(2):
                first = (layer * 2 + g) * 56 + q * 14
                here = (out >= first) & (out < first + 14)
                source = jnp.where(here, q * 56 + layer * 28 + g + 2 * (out - first), source)
    pick = (inn == source).astype(jnp.bfloat16)
    for i, s in enumerate(LATE):
        for a in range(2):
            for b in range(2):
                held[place(a, s, b)] = late[2 * i + b][a, b]
    for copy in copies:
        copy.wait()
    copies = []
    for n in range(8):
        rows = held[n].reshape(224, 512)
        moved = jnp.dot(pick, rows, preferred_element_type=jnp.float32).astype(jnp.bfloat16)
        for layer in range(2):
            for g in range(2):
                first = (layer * 2 + g) * 56
                rows_out[n, g, layer] = moved[first : first + 56]
        for g, target in enumerate((gate_hbm, up_hbm)):
            copy = pltpu.make_async_copy(rows_out.at[n, g], target.at[:, pl.ds(56 * n, 56)], out_sems.at[2 * n + g])
            copy.start()
            copies.append(copy)
    for copy in copies:
        copy.wait()


def unpack(early, late):
    return pl.pallas_call(
        unpack_kernel,
        out_shape=[hbm(2, 448, 512)] * 2,
        in_specs=[INHBM] * 2 + [ANYWHERE] * 2 + [INHBM] * 10 + [WHOLE] * 8,
        out_specs=[INHBM] * 2,
        scratch_shapes=[
            pltpu.VMEM((8, 2, 2, 56, 512), jnp.bfloat16),
            pltpu.VMEM((8, 2, 2, 56, 512), jnp.bfloat16),
            pltpu.SemaphoreType.DMA((16,)),
            pltpu.SemaphoreType.DMA((16,)),
        ],
        compiler_params=params(10),
        name="unpack",
    )(*map(outside, early[:2]), *early[2:4], *map(outside, early[4:]), *map(inside, late))


def halve_kernel(p0, p1, p2, p3, keep, give):
    h = lax.axis_index("xhi")
    keep[...] = (p0[h] + p1[h]) + (p2[h] + p3[h])
    give[...] = (p0[1 - h] + p1[1 - h]) + (p2[1 - h] + p3[1 - h])


def halve(parts):
    return pl.pallas_call(
        halve_kernel,
        out_shape=[vmem(2, 16, 896, dtype=jnp.float32)] * 2,
        in_specs=[WHOLE] * 4,
        out_specs=[WHOLE] * 2,
        compiler_params=params(8),
        name="halve",
    )(inside(parts[0]), *parts[1:])


def gated_kernel(keep, came, out_ref):
    total = (keep[...] + came[...]).reshape(32, 896)
    up = pltpu.roll(total, 896 - 32, 1)
    turned = (total / (1.0 + jnp.exp(-total)) * up).T
    quads = []
    for q in range(4):
        blocks = [turned[64 * i : 64 * i + 32] if i < 14 else jnp.zeros((32, 32), jnp.float32) for i in range(4 * q, 4 * q + 4)]
        quads.append(jnp.concatenate(blocks, axis=1))
    rows = jnp.concatenate(quads, axis=0).astype(jnp.bfloat16)
    to = lax.broadcasted_iota(jnp.int32, (128, 128), 0)
    of = lax.broadcasted_iota(jnp.int32, (128, 128), 1)
    pick = (of == ((to & 3) << 5) + (to >> 2)).astype(jnp.bfloat16)
    out_ref[...] = jnp.dot(pick, rows, preferred_element_type=jnp.float32).astype(jnp.bfloat16)


def gated(keep, came):
    return pl.pallas_call(
        gated_kernel,
        out_shape=jax.ShapeDtypeStruct((128, 128), jnp.bfloat16),
        in_specs=[WHOLE] * 2,
        out_specs=WHOLE,
        compiler_params=params(8),
        name="gated",
    )(inside(keep), inside(came))


def final_kernel(came, out_ref):
    turned = came[...].astype(jnp.float32).T.astype(jnp.bfloat16)
    of = lax.broadcasted_iota(jnp.int32, (128, 448), 0)
    to = lax.broadcasted_iota(jnp.int32, (128, 448), 1)
    total = jnp.zeros((32, 448), jnp.float32)
    for i in range(4):
        unit = ((of & 3) << 2) + i
        pick = ((to == (of >> 2) * 14 + unit) & (unit < 14)).astype(jnp.bfloat16)
        total += jnp.dot(turned[32 * i : 32 * i + 32], pick, preferred_element_type=jnp.float32)
    out_ref[...] = total.astype(jnp.bfloat16).reshape(2, 16, 448)


def final(came):
    return pl.pallas_call(
        final_kernel,
        out_shape=jax.ShapeDtypeStruct((2, 16, 448), jnp.bfloat16),
        in_specs=[WHOLE],
        out_specs=WHOLE,
        compiler_params=params(8),
        name="final",
    )(came)


def send(piece, a, s, b):
    return lax.ppermute(piece, ROW, hop(a, s, b))


def side(piece, h, y):
    pairs = [(p * 4 + q, (p ^ h) * 4 + (q + y) % 4) for p in range(2) for q in range(4)]
    return lax.ppermute(piece, COL, pairs)


def body(joined, probes):
    w = joined.reshape(2, 32, 28, 512).transpose(0, 2, 1, 3).reshape(56, 32, 512)
    *outs, w = pack_first(w)
    rest = pack_second(w, probes)
    outs, parts = [*outs, *rest[:8]], rest[8:]
    early = [send(piece, 0, s, 0) for s, piece in zip(EARLY, outs)]
    across = [send(piece, a, 4, 0) for a, piece in zip((0, 1), outs[2:4])]
    crossed = send(outs[4], 1, 0, 0)
    parts = [parts[0]] + [side(parts[s], 0, s) for s in range(1, 4)]
    keep, give = halve(parts)
    came = side(give, 1, 0)
    joins = join(crossed, outs[5:9])
    late = [send(piece, 0, s, 0) for s, piece in zip(LATE, joins)]
    post = gather(early)
    post = send(post, 1, 0, 0)
    mine = early + across + [post, crossed] + late + [outs[9]]
    other = [send(piece, 0, 0, 1) for piece in mine]
    hid = gated(keep, came).reshape(32, 4, 128)
    hid = lax.all_to_all(hid, ROW, 0, 0, tiled=True)
    hid = final(hid.reshape(128, 128))
    both = [piece for pair in zip(mine, other) for piece in pair]
    gate_rows, up_rows = unpack(both[20:22] + both[10:12] + both[0:10], both[12:20])
    return gate_rows, up_rows, hid


def solution(mesh):
    split = Mesh(mesh.devices.reshape(NX, NZ, NC, 2, 4), ROW + COL)
    return jax.shard_map(
        body,
        mesh=split,
        in_specs=(P(None, None, ROW, None, COL), P(None, None, COL)),
        out_specs=(P(None, ROW, COL), P(None, ROW, COL), P(None, COL, ROW)),
        check_vma=False,
    )
```

```python
import jax
import jax.numpy as jnp
from jax import lax
from jax.experimental import pallas as pl
from jax.experimental.pallas import tpu as pltpu
from jax.sharding import Mesh
from jax.sharding import PartitionSpec as P

ROW = ("xlo", "z", "core")
COL = ("xhi", "y")
NX, NZ, NC = 2, 8, 2
EARLY = (3, 5)
LATE = (2, 6, 1, 7)
FLIPPED = (0,) + LATE
PIECES = tuple((a, s) for s in EARLY for a in (0, 1)) + ((0, 4), (1, 4)) + tuple((1, s) for s in FLIPPED) + tuple((0, s) for s in LATE) + ((0, 0),)
FIRST = PIECES[:4] + PIECES[6:11]
SECOND = PIECES[4:6] + PIECES[11:]
PIECE = (56, 512)


def row_index(x, z, c):
    return (x * NZ + z) * NC + c


def hop(a, s, b):
    return [
        (row_index(x, z, c), row_index(x ^ a, (z + s) % NZ, c ^ b))
        for x in range(NX)
        for z in range(NZ)
        for c in range(NC)
    ]


def vmem(*shape, dtype=jnp.bfloat16):
    return pltpu.VMEM(shape, dtype)


def hbm(*shape, dtype=jnp.bfloat16):
    return pltpu.HBM(shape, dtype)


def inside(x):
    return pltpu.with_memory_space_constraint(x, pltpu.VMEM)


def outside(x):
    return pltpu.with_memory_space_constraint(x, pltpu.HBM)


WHOLE = pl.BlockSpec(memory_space=pltpu.VMEM)
ANYWHERE = pl.BlockSpec(memory_space=pl.ANY)
INHBM = pl.BlockSpec(memory_space=pltpu.HBM)


def params(mib):
    return pltpu.CompilerParams(vmem_limit_bytes=mib << 20)


def selection(pieces):
    x, z, c = lax.axis_index("xlo"), lax.axis_index("z"), lax.axis_index("core")
    row = lax.broadcasted_iota(jnp.int32, (16 * len(pieces), 256), 0)
    column = lax.broadcasted_iota(jnp.int32, (16 * len(pieces), 256), 1)
    j, b, n = row & 7, (row >> 3) & 1, row >> 4
    flip, step = jnp.zeros_like(n), jnp.zeros_like(n)
    for i, (a, s) in enumerate(pieces):
        flip = jnp.where(n == i, a, flip)
        step = jnp.where(n == i, s, step)
    block = ((flip ^ x) << 4) + (((z + step) & 7) << 1) + (b ^ c)
    return (column == (j << 5) + block).astype(jnp.bfloat16)


def pack_first_kernel(w_hbm, *refs):
    outs, w, sems = refs[:3], refs[3], refs[4]
    copies = [pltpu.make_async_copy(w_hbm.at[pl.ds(8 * g, 8)], w.at[pl.ds(8 * g, 8)], sems.at[g]) for g in range(7)]
    for copy in copies:
        copy.start()
    pick = selection(FIRST)
    for g in range(7):
        copies[g].wait()
        rows = w[8 * g : 8 * g + 8].reshape(256, 512)
        moved = jnp.dot(pick, rows, preferred_element_type=jnp.float32).astype(jnp.bfloat16)
        moved = moved.reshape(9, 2, 8, 512)
        for out, first, count in zip(outs, (0, 2, 4), (2, 2, 5)):
            out[:, :, 8 * g : 8 * g + 8, :] = moved[first : first + count]


def pack_first(w):
    return pl.pallas_call(
        pack_first_kernel,
        out_shape=[vmem(2, 2, *PIECE)] * 2 + [vmem(5, 2, *PIECE), vmem(56, 32, 512)],
        in_specs=[INHBM],
        out_specs=[WHOLE] * 4,
        scratch_shapes=[pltpu.SemaphoreType.DMA((7,))],
        compiler_params=params(4),
        name="pack_first",
    )(outside(w))


def pack_second_kernel(w, probes_hbm, *refs):
    outs, parts, (held, probes, proj, sems, out_sems, part_sems) = refs[:7], refs[7:11], refs[11:]
    y = lax.axis_index("y")
    first = pltpu.make_async_copy(probes_hbm, probes, sems.at[0])
    first.start()
    pick = selection(SECOND)
    dims = (((1,), (1,)), ((), ()))
    sent = []

    def ship(half, begin, count):
        rows = pl.ds(begin, count)
        pairs = [(held.at[i, :, rows], outs[i].at[:, rows]) for i in range(2)]
        pairs += [(held.at[2 + i, :, rows], outs[2 + i].at[0, :, rows]) for i in range(4)]
        pairs.append((held.at[6, :, rows], outs[6].at[:, rows]))
        for i, (source, target) in enumerate(pairs):
            sent.append(pltpu.make_async_copy(source, target, out_sems.at[7 * half + i]))
            sent[-1].start()

    for layer in range(2):
        part = w[28 * layer : 28 * layer + 28].reshape(896, 512)
        if layer == 0:
            first.wait()
        product = lax.dot_general(probes[layer], part, dims, preferred_element_type=jnp.float32)
        proj[layer] = product.reshape(8, 16, 896)
        for s in range(1, 4):
            for h in range(2):
                n = len(sent)
                source = proj.at[layer, 4 * h + ((y + s) & 3)]
                sent.append(pltpu.make_async_copy(source, parts[s].at[h, layer], part_sems.at[n]))
                sent[-1].start()
        for h in range(2):
            parts[0][h, layer] = proj[layer, 4 * h + y]
    for g in range(7):
        rows = w[8 * g : 8 * g + 8].reshape(256, 512)
        moved = jnp.dot(pick, rows, preferred_element_type=jnp.float32).astype(jnp.bfloat16)
        held[:, :, 8 * g : 8 * g + 8, :] = moved.reshape(7, 2, 8, 512)
        if g == 3:
            ship(0, 0, 32)
    ship(1, 32, 24)
    for copy in sent:
        copy.wait()


def pack_second(w, probes):
    return pl.pallas_call(
        pack_second_kernel,
        out_shape=[hbm(2, *PIECE)] * 2
        + [hbm(2, 2, *PIECE)] * 4
        + [hbm(2, *PIECE)]
        + [vmem(2, 2, 16, 896, dtype=jnp.float32)]
        + [hbm(2, 2, 16, 896, dtype=jnp.float32)] * 3,
        in_specs=[WHOLE, INHBM],
        out_specs=[INHBM] * 7 + [WHOLE] + [INHBM] * 3,
        scratch_shapes=[
            pltpu.VMEM((7, 2, 56, 512), jnp.bfloat16),
            pltpu.VMEM((2, 128, 512), jnp.bfloat16),
            pltpu.VMEM((2, 8, 16, 896), jnp.float32),
            pltpu.SemaphoreType.DMA((1,)),
            pltpu.SemaphoreType.DMA((14,)),
            pltpu.SemaphoreType.DMA((12,)),
        ],
        compiler_params=params(8),
        name="pack_second",
    )(inside(w), outside(probes))


def join_kernel(crossed, *refs):
    outs, near, sems = refs[4:8], refs[8], refs[9]
    copies = [pltpu.make_async_copy(crossed.at[1 + n], out.at[1], sems.at[n]) for n, out in enumerate(outs)]
    for copy in copies:
        copy.start()
    near[...] = crossed[0]
    for copy in copies:
        copy.wait()


def join(crossed, straight):
    return pl.pallas_call(
        join_kernel,
        out_shape=[hbm(2, 2, *PIECE)] * 4 + [vmem(2, *PIECE)],
        in_specs=[WHOLE] + [INHBM] * 4,
        out_specs=[INHBM] * 4 + [WHOLE],
        scratch_shapes=[pltpu.SemaphoreType.DMA((4,))],
        input_output_aliases={1: 0, 2: 1, 3: 2, 4: 3},
        compiler_params=params(1),
        name="join",
    )(inside(crossed), *map(outside, straight))


def gather_kernel(*refs):
    pieces, out, sems = refs[:2], refs[2], refs[3]
    copies = [pltpu.make_async_copy(piece.at[1], out.at[n], sems.at[n]) for n, piece in enumerate(pieces)]
    for copy in copies:
        copy.start()
    for copy in copies:
        copy.wait()


def gather(pieces):
    return pl.pallas_call(
        gather_kernel,
        out_shape=vmem(2, 2, *PIECE),
        in_specs=[ANYWHERE] * 2,
        out_specs=WHOLE,
        scratch_shapes=[pltpu.SemaphoreType.DMA((2,))],
        compiler_params=params(1),
        name="gather",
    )(*pieces)


def unpack_kernel(*refs):
    early, late, (gate_hbm, up_hbm, held, rows_out, sems, out_sems) = refs[:14], refs[14:22], refs[22:]
    x, z, c = lax.axis_index("xlo"), lax.axis_index("z"), lax.axis_index("core")
    local, crossed, z3, z5, d04, d14, post = early[0:2], early[2:4], early[4:6], early[6:8], early[8:10], early[10:12], early[12:14]
    pieces = []
    for b in range(2):
        pieces += [(local[b].at[b], 0, 0, b), (crossed[b].at[b], 1, 0, b)]
        pieces += [(z3[b].at[0, b], 0, 3, b), (post[b].at[0, b], 1, 3, b)]
        pieces += [(z5[b].at[0, b], 0, 5, b), (post[b].at[1, b], 1, 5, b)]
        pieces += [(d04[b].at[b], 0, 4, b), (d14[b].at[b], 1, 4, b)]

    def place(a, s, b):
        return (a ^ x) * 4 + (((z - s) & 7) >> 1), (z - s) & 1, b ^ c

    copies = []
    for source, a, s, b in pieces:
        copies.append(pltpu.make_async_copy(source, held.at[place(a, s, b)], sems.at[len(copies)]))
        copies[-1].start()
    out = lax.broadcasted_iota(jnp.int32, (224, 224), 0)
    inn = lax.broadcasted_iota(jnp.int32, (224, 224), 1)
    source = jnp.zeros((224, 224), jnp.int32)
    for q in range(4):
        for layer in range(2):
            for g in range(2):
                first = (layer * 2 + g) * 56 + q * 14
                here = (out >= first) & (out < first + 14)
                source = jnp.where(here, q * 56 + layer * 28 + g + 2 * (out - first), source)
    pick = (inn == source).astype(jnp.bfloat16)
    for i, s in enumerate(LATE):
        for a in range(2):
            for b in range(2):
                held[place(a, s, b)] = late[2 * i + b][a, b]
    for copy in copies:
        copy.wait()
    copies = []
    for n in range(8):
        rows = held[n].reshape(224, 512)
        moved = jnp.dot(pick, rows, preferred_element_type=jnp.float32).astype(jnp.bfloat16)
        for layer in range(2):
            for g in range(2):
                first = (layer * 2 + g) * 56
                rows_out[n, g, layer] = moved[first : first + 56]
        for g, target in enumerate((gate_hbm, up_hbm)):
            copy = pltpu.make_async_copy(rows_out.at[n, g], target.at[:, pl.ds(56 * n, 56)], out_sems.at[2 * n + g])
            copy.start()
            copies.append(copy)
    for copy in copies:
        copy.wait()


def unpack(early, late):
    return pl.pallas_call(
        unpack_kernel,
        out_shape=[hbm(2, 448, 512)] * 2,
        in_specs=[INHBM] * 2 + [ANYWHERE] * 2 + [INHBM] * 10 + [WHOLE] * 8,
        out_specs=[INHBM] * 2,
        scratch_shapes=[
            pltpu.VMEM((8, 2, 2, 56, 512), jnp.bfloat16),
            pltpu.VMEM((8, 2, 2, 56, 512), jnp.bfloat16),
            pltpu.SemaphoreType.DMA((16,)),
            pltpu.SemaphoreType.DMA((16,)),
        ],
        compiler_params=params(10),
        name="unpack",
    )(*map(outside, early[:2]), *early[2:4], *map(outside, early[4:]), *map(inside, late))


def halve_kernel(p0, p1, p2, p3, keep, give):
    h = lax.axis_index("xhi")
    keep[...] = (p0[h] + p1[h]) + (p2[h] + p3[h])
    give[...] = (p0[1 - h] + p1[1 - h]) + (p2[1 - h] + p3[1 - h])


def halve(parts):
    return pl.pallas_call(
        halve_kernel,
        out_shape=[vmem(2, 16, 896, dtype=jnp.float32)] * 2,
        in_specs=[WHOLE] * 4,
        out_specs=[WHOLE] * 2,
        compiler_params=params(8),
        name="halve",
    )(inside(parts[0]), *parts[1:])


def gated_kernel(keep, came, out_ref):
    total = (keep[...] + came[...]).reshape(32, 896)
    up = pltpu.roll(total, 896 - 32, 1)
    turned = (total / (1.0 + jnp.exp(-total)) * up).T
    quads = []
    for q in range(4):
        blocks = [turned[64 * i : 64 * i + 32] if i < 14 else jnp.zeros((32, 32), jnp.float32) for i in range(4 * q, 4 * q + 4)]
        quads.append(jnp.concatenate(blocks, axis=1))
    rows = jnp.concatenate(quads, axis=0).astype(jnp.bfloat16)
    to = lax.broadcasted_iota(jnp.int32, (128, 128), 0)
    of = lax.broadcasted_iota(jnp.int32, (128, 128), 1)
    pick = (of == ((to & 3) << 5) + (to >> 2)).astype(jnp.bfloat16)
    out_ref[...] = jnp.dot(pick, rows, preferred_element_type=jnp.float32).astype(jnp.bfloat16)


def gated(keep, came):
    return pl.pallas_call(
        gated_kernel,
        out_shape=jax.ShapeDtypeStruct((128, 128), jnp.bfloat16),
        in_specs=[WHOLE] * 2,
        out_specs=WHOLE,
        compiler_params=params(8),
        name="gated",
    )(inside(keep), inside(came))


def final_kernel(came, out_ref):
    turned = came[...].astype(jnp.float32).T.astype(jnp.bfloat16)
    of = lax.broadcasted_iota(jnp.int32, (128, 512), 0)
    to = lax.broadcasted_iota(jnp.int32, (128, 512), 1)
    pick = (to == (of >> 2) * 14 + ((of & 3) << 2)).astype(jnp.bfloat16)
    spread = jnp.dot(turned, pick, preferred_element_type=jnp.float32)
    total = spread[:32]
    for i in range(1, 4):
        total += pltpu.roll(spread[32 * i : 32 * i + 32], i, 1)
    out_ref[...] = total[:, :448].astype(jnp.bfloat16).reshape(2, 16, 448)


def final(came):
    return pl.pallas_call(
        final_kernel,
        out_shape=jax.ShapeDtypeStruct((2, 16, 448), jnp.bfloat16),
        in_specs=[WHOLE],
        out_specs=WHOLE,
        compiler_params=params(8),
        name="final",
    )(came)


def send(piece, a, s, b):
    return lax.ppermute(piece, ROW, hop(a, s, b))


def side(piece, h, y):
    pairs = [(p * 4 + q, (p ^ h) * 4 + (q + y) % 4) for p in range(2) for q in range(4)]
    return lax.ppermute(piece, COL, pairs)


def body(joined, probes):
    w = joined.reshape(2, 32, 28, 512).transpose(0, 2, 1, 3).reshape(56, 32, 512)
    *outs, w = pack_first(w)
    rest = pack_second(w, probes)
    outs, parts = [*outs[:2], *rest[:2], outs[2], *rest[2:7]], rest[7:]
    early = [send(piece, 0, s, 0) for s, piece in zip(EARLY, outs)]
    across = [send(piece, a, 4, 0) for a, piece in zip((0, 1), outs[2:4])]
    crossed = send(outs[4], 1, 0, 0)
    parts = [parts[0]] + [side(parts[s], 0, s) for s in range(1, 4)]
    keep, give = halve(parts)
    came = side(give, 1, 0)
    *joins, near = join(crossed, outs[5:9])
    late = [send(piece, 0, s, 0) for s, piece in zip(LATE, joins)]
    post = gather(early)
    post = send(post, 1, 0, 0)
    mine = early + across + [post, near] + late + [outs[9]]
    other = [send(piece, 0, 0, 1) for piece in mine]
    hid = gated(keep, came).reshape(32, 4, 128)
    hid = lax.all_to_all(hid, ROW, 0, 0, tiled=True)
    hid = final(hid.reshape(128, 128))
    both = [piece for pair in zip(mine, other) for piece in pair]
    gate_rows, up_rows = unpack(both[20:22] + both[10:12] + both[0:10], both[12:20])
    return gate_rows, up_rows, hid


def solution(mesh):
    split = Mesh(mesh.devices.reshape(NX, NZ, NC, 2, 4), ROW + COL)
    return jax.shard_map(
        body,
        mesh=split,
        in_specs=(P(None, None, ROW, None, COL), P(None, None, COL)),
        out_specs=(P(None, ROW, COL), P(None, ROW, COL), P(None, COL, ROW)),
        check_vma=False,
    )
```

```python
import jax
import jax.numpy as jnp
from jax import lax
from jax.experimental import pallas as pl
from jax.experimental.pallas import tpu as pltpu
from jax.sharding import Mesh
from jax.sharding import PartitionSpec as P

ROW = ("xlo", "z", "core")
COL = ("xhi", "y")
NX, NZ, NC = 2, 8, 2
EARLY = (3, 5)
LATE = (2, 6, 1, 7)
FLIPPED = (0,) + LATE
PIECES = tuple((a, s) for s in EARLY for a in (0, 1)) + ((0, 4), (1, 4)) + tuple((1, s) for s in FLIPPED) + tuple((0, s) for s in LATE) + ((0, 0),)
FIRST = PIECES[:4] + PIECES[6:11]
SECOND = PIECES[4:6] + PIECES[11:]
PIECE = (56, 512)


def row_index(x, z, c):
    return (x * NZ + z) * NC + c


def hop(a, s, b):
    return [
        (row_index(x, z, c), row_index(x ^ a, (z + s) % NZ, c ^ b))
        for x in range(NX)
        for z in range(NZ)
        for c in range(NC)
    ]


def vmem(*shape, dtype=jnp.bfloat16):
    return pltpu.VMEM(shape, dtype)


def hbm(*shape, dtype=jnp.bfloat16):
    return pltpu.HBM(shape, dtype)


def inside(x):
    return pltpu.with_memory_space_constraint(x, pltpu.VMEM)


def outside(x):
    return pltpu.with_memory_space_constraint(x, pltpu.HBM)


WHOLE = pl.BlockSpec(memory_space=pltpu.VMEM)
ANYWHERE = pl.BlockSpec(memory_space=pl.ANY)
INHBM = pl.BlockSpec(memory_space=pltpu.HBM)


def params(mib):
    return pltpu.CompilerParams(vmem_limit_bytes=mib << 20)


def selection(pieces):
    x, z, c = lax.axis_index("xlo"), lax.axis_index("z"), lax.axis_index("core")
    row = lax.broadcasted_iota(jnp.int32, (16 * len(pieces), 256), 0)
    column = lax.broadcasted_iota(jnp.int32, (16 * len(pieces), 256), 1)
    j, b, n = row & 7, (row >> 3) & 1, row >> 4
    flip, step = jnp.zeros_like(n), jnp.zeros_like(n)
    for i, (a, s) in enumerate(pieces):
        flip = jnp.where(n == i, a, flip)
        step = jnp.where(n == i, s, step)
    block = ((flip ^ x) << 4) + (((z + step) & 7) << 1) + (b ^ c)
    return (column == (j << 5) + block).astype(jnp.bfloat16)


def pack_first_kernel(w_hbm, *refs):
    outs, w, sems = refs[:3], refs[3], refs[4]
    copies = [pltpu.make_async_copy(w_hbm.at[pl.ds(8 * g, 8)], w.at[pl.ds(8 * g, 8)], sems.at[g]) for g in range(7)]
    for copy in copies:
        copy.start()
    pick = selection(FIRST)
    for g in range(7):
        copies[g].wait()
        rows = w[8 * g : 8 * g + 8].reshape(256, 512)
        moved = jnp.dot(pick, rows, preferred_element_type=jnp.float32).astype(jnp.bfloat16)
        moved = moved.reshape(9, 2, 8, 512)
        for out, first, count in zip(outs, (0, 2, 4), (2, 2, 5)):
            out[:, :, 8 * g : 8 * g + 8, :] = moved[first : first + count]


def pack_first(w):
    return pl.pallas_call(
        pack_first_kernel,
        out_shape=[vmem(2, 2, *PIECE)] * 2 + [vmem(5, 2, *PIECE), vmem(56, 32, 512)],
        in_specs=[INHBM],
        out_specs=[WHOLE] * 4,
        scratch_shapes=[pltpu.SemaphoreType.DMA((7,))],
        compiler_params=params(4),
        name="pack_first",
    )(outside(w))


def pack_second_kernel(w, probes_hbm, *refs):
    outs, parts, (held, probes, proj, sems, out_sems, part_sems) = refs[:7], refs[7:11], refs[11:]
    y = lax.axis_index("y")
    first = pltpu.make_async_copy(probes_hbm, probes, sems.at[0])
    first.start()
    pick = selection(SECOND)
    dims = (((1,), (1,)), ((), ()))
    sent = []

    def ship(half, begin, count):
        rows = pl.ds(begin, count)
        pairs = [(held.at[i, :, rows], outs[i].at[:, rows]) for i in range(2)]
        pairs += [(held.at[2 + i, :, rows], outs[2 + i].at[0, :, rows]) for i in range(4)]
        pairs.append((held.at[6, :, rows], outs[6].at[:, rows]))
        for i, (source, target) in enumerate(pairs):
            sent.append(pltpu.make_async_copy(source, target, out_sems.at[7 * half + i]))
            sent[-1].start()

    for layer in range(2):
        part = w[28 * layer : 28 * layer + 28].reshape(896, 512)
        if layer == 0:
            first.wait()
        product = lax.dot_general(probes[layer], part, dims, preferred_element_type=jnp.float32)
        proj[layer] = product.reshape(8, 16, 896)
        for s in range(1, 4):
            for h in range(2):
                n = len(sent)
                source = proj.at[layer, 4 * h + ((y + s) & 3)]
                sent.append(pltpu.make_async_copy(source, parts[s].at[h, layer], part_sems.at[n]))
                sent[-1].start()
        for h in range(2):
            parts[0][h, layer] = proj[layer, 4 * h + y]
    for g in range(7):
        rows = w[8 * g : 8 * g + 8].reshape(256, 512)
        moved = jnp.dot(pick, rows, preferred_element_type=jnp.float32).astype(jnp.bfloat16)
        held[:, :, 8 * g : 8 * g + 8, :] = moved.reshape(7, 2, 8, 512)
        if g == 3:
            ship(0, 0, 32)
    ship(1, 32, 24)
    for copy in sent:
        copy.wait()


def pack_second(w, probes):
    return pl.pallas_call(
        pack_second_kernel,
        out_shape=[hbm(2, *PIECE)] * 2
        + [hbm(2, 2, *PIECE)] * 4
        + [hbm(2, *PIECE)]
        + [vmem(2, 2, 16, 896, dtype=jnp.float32)]
        + [hbm(2, 2, 16, 896, dtype=jnp.float32)] * 3,
        in_specs=[WHOLE, INHBM],
        out_specs=[INHBM] * 7 + [WHOLE] + [INHBM] * 3,
        scratch_shapes=[
            pltpu.VMEM((7, 2, 56, 512), jnp.bfloat16),
            pltpu.VMEM((2, 128, 512), jnp.bfloat16),
            pltpu.VMEM((2, 8, 16, 896), jnp.float32),
            pltpu.SemaphoreType.DMA((1,)),
            pltpu.SemaphoreType.DMA((14,)),
            pltpu.SemaphoreType.DMA((12,)),
        ],
        compiler_params=params(8),
        name="pack_second",
    )(inside(w), outside(probes))


def join_kernel(crossed, *refs):
    outs, near, sems = refs[4:8], refs[8], refs[9]
    copies = [pltpu.make_async_copy(crossed.at[1 + n], out.at[1], sems.at[n]) for n, out in enumerate(outs)]
    for copy in copies:
        copy.start()
    near[...] = crossed[0]
    for copy in copies:
        copy.wait()


def join(crossed, straight):
    return pl.pallas_call(
        join_kernel,
        out_shape=[hbm(2, 2, *PIECE)] * 4 + [vmem(2, *PIECE)],
        in_specs=[WHOLE] + [INHBM] * 4,
        out_specs=[INHBM] * 4 + [WHOLE],
        scratch_shapes=[pltpu.SemaphoreType.DMA((4,))],
        input_output_aliases={1: 0, 2: 1, 3: 2, 4: 3},
        compiler_params=params(1),
        name="join",
    )(inside(crossed), *map(outside, straight))


def gather_kernel(*refs):
    pieces, out, sems = refs[:2], refs[2], refs[3]
    copies = [pltpu.make_async_copy(piece.at[1], out.at[n], sems.at[n]) for n, piece in enumerate(pieces)]
    for copy in copies:
        copy.start()
    for copy in copies:
        copy.wait()


def gather(pieces):
    return pl.pallas_call(
        gather_kernel,
        out_shape=vmem(2, 2, *PIECE),
        in_specs=[ANYWHERE] * 2,
        out_specs=WHOLE,
        scratch_shapes=[pltpu.SemaphoreType.DMA((2,))],
        compiler_params=params(1),
        name="gather",
    )(*pieces)


def unpack_kernel(*refs):
    early, late, (gate_hbm, up_hbm, held, rows_out, out_sems) = refs[:14], refs[14:22], refs[22:]
    x, z, c = lax.axis_index("xlo"), lax.axis_index("z"), lax.axis_index("core")
    local, crossed, z3, z5, d04, d14, post = early[0:2], early[2:4], early[4:6], early[6:8], early[8:10], early[10:12], early[12:14]
    pieces = []
    for b in range(2):
        pieces += [(local[b].at[b], 0, 0, b), (crossed[b].at[b], 1, 0, b)]
        pieces += [(z3[b].at[0, b], 0, 3, b), (post[b].at[0, b], 1, 3, b)]
        pieces += [(z5[b].at[0, b], 0, 5, b), (post[b].at[1, b], 1, 5, b)]
        pieces += [(d04[b].at[b], 0, 4, b), (d14[b].at[b], 1, 4, b)]

    def place(a, s, b):
        return (a ^ x) * 4 + (((z - s) & 7) >> 1), (z - s) & 1, b ^ c

    out = lax.broadcasted_iota(jnp.int32, (224, 224), 0)
    inn = lax.broadcasted_iota(jnp.int32, (224, 224), 1)
    source = jnp.zeros((224, 224), jnp.int32)
    for q in range(4):
        for layer in range(2):
            for g in range(2):
                first = (layer * 2 + g) * 56 + q * 14
                here = (out >= first) & (out < first + 14)
                source = jnp.where(here, q * 56 + layer * 28 + g + 2 * (out - first), source)
    pick = (inn == source).astype(jnp.bfloat16)
    for i, s in enumerate(LATE):
        for a in range(2):
            for b in range(2):
                held[place(a, s, b)] = late[2 * i + b][a, b]
    for source, a, s, b in pieces:
        held[place(a, s, b)] = source[...]
    copies = []
    for n in range(8):
        rows = held[n].reshape(224, 512)
        moved = jnp.dot(pick, rows, preferred_element_type=jnp.float32).astype(jnp.bfloat16)
        for layer in range(2):
            for g in range(2):
                first = (layer * 2 + g) * 56
                rows_out[n, g, layer] = moved[first : first + 56]
        for g, target in enumerate((gate_hbm, up_hbm)):
            copy = pltpu.make_async_copy(rows_out.at[n, g], target.at[:, pl.ds(56 * n, 56)], out_sems.at[2 * n + g])
            copy.start()
            copies.append(copy)
    for copy in copies:
        copy.wait()


def unpack(early, late):
    return pl.pallas_call(
        unpack_kernel,
        out_shape=[hbm(2, 448, 512)] * 2,
        in_specs=[WHOLE] * 22,
        out_specs=[INHBM] * 2,
        scratch_shapes=[
            pltpu.VMEM((8, 2, 2, 56, 512), jnp.bfloat16),
            pltpu.VMEM((8, 2, 2, 56, 512), jnp.bfloat16),
            pltpu.SemaphoreType.DMA((16,)),
        ],
        compiler_params=params(10),
        name="unpack",
    )(*map(inside, early), *map(inside, late))


def halve_kernel(p0, p1, p2, p3, keep, give):
    h = lax.axis_index("xhi")
    keep[...] = (p0[h] + p1[h]) + (p2[h] + p3[h])
    give[...] = (p0[1 - h] + p1[1 - h]) + (p2[1 - h] + p3[1 - h])


def halve(parts):
    return pl.pallas_call(
        halve_kernel,
        out_shape=[vmem(2, 16, 896, dtype=jnp.float32)] * 2,
        in_specs=[WHOLE] * 4,
        out_specs=[WHOLE] * 2,
        compiler_params=params(8),
        name="halve",
    )(inside(parts[0]), *parts[1:])


def gated_kernel(keep, came, out_ref):
    total = (keep[...] + came[...]).reshape(32, 896)
    up = pltpu.roll(total, 896 - 32, 1)
    turned = (total / (1.0 + jnp.exp(-total)) * up).T
    quads = []
    for q in range(4):
        blocks = [turned[64 * i : 64 * i + 32] if i < 14 else jnp.zeros((32, 32), jnp.float32) for i in range(4 * q, 4 * q + 4)]
        quads.append(jnp.concatenate(blocks, axis=1))
    rows = jnp.concatenate(quads, axis=0).astype(jnp.bfloat16)
    to = lax.broadcasted_iota(jnp.int32, (128, 128), 0)
    of = lax.broadcasted_iota(jnp.int32, (128, 128), 1)
    pick = (of == ((to & 3) << 5) + (to >> 2)).astype(jnp.bfloat16)
    out_ref[...] = jnp.dot(pick, rows, preferred_element_type=jnp.float32).astype(jnp.bfloat16)


def gated(keep, came):
    return pl.pallas_call(
        gated_kernel,
        out_shape=jax.ShapeDtypeStruct((128, 128), jnp.bfloat16),
        in_specs=[WHOLE] * 2,
        out_specs=WHOLE,
        compiler_params=params(8),
        name="gated",
    )(inside(keep), inside(came))


def final_kernel(came, out_ref):
    turned = came[...].astype(jnp.float32).T.astype(jnp.bfloat16)
    of = lax.broadcasted_iota(jnp.int32, (128, 512), 0)
    to = lax.broadcasted_iota(jnp.int32, (128, 512), 1)
    pick = (to == (of >> 2) * 14 + ((of & 3) << 2)).astype(jnp.bfloat16)
    spread = jnp.dot(turned, pick, preferred_element_type=jnp.float32)
    total = spread[:32]
    for i in range(1, 4):
        total += pltpu.roll(spread[32 * i : 32 * i + 32], i, 1)
    out_ref[...] = total[:, :448].astype(jnp.bfloat16).reshape(2, 16, 448)


def final(came):
    return pl.pallas_call(
        final_kernel,
        out_shape=jax.ShapeDtypeStruct((2, 16, 448), jnp.bfloat16),
        in_specs=[WHOLE],
        out_specs=WHOLE,
        compiler_params=params(8),
        name="final",
    )(came)


def send(piece, a, s, b):
    return lax.ppermute(piece, ROW, hop(a, s, b))


def side(piece, h, y):
    pairs = [(p * 4 + q, (p ^ h) * 4 + (q + y) % 4) for p in range(2) for q in range(4)]
    return lax.ppermute(piece, COL, pairs)


def body(joined, probes):
    w = joined.reshape(2, 32, 28, 512).transpose(0, 2, 1, 3).reshape(56, 32, 512)
    *outs, w = pack_first(w)
    rest = pack_second(w, probes)
    outs, parts = [*outs[:2], *rest[:2], outs[2], *rest[2:7]], rest[7:]
    early = [send(piece, 0, s, 0) for s, piece in zip(EARLY, outs)]
    across = [send(piece, a, 4, 0) for a, piece in zip((0, 1), outs[2:4])]
    crossed = send(outs[4], 1, 0, 0)
    parts = [parts[0]] + [side(parts[s], 0, s) for s in range(1, 4)]
    keep, give = halve(parts)
    came = side(give, 1, 0)
    *joins, near = join(crossed, outs[5:9])
    late = [send(piece, 0, s, 0) for s, piece in zip(LATE, joins)]
    post = gather(early)
    post = send(post, 1, 0, 0)
    mine = early + across + [post, near] + late + [outs[9]]
    other = [send(piece, 0, 0, 1) for piece in mine]
    hid = gated(keep, came).reshape(32, 4, 128)
    hid = lax.all_to_all(hid, ROW, 0, 0, tiled=True)
    hid = final(hid.reshape(128, 128))
    both = [piece for pair in zip(mine, other) for piece in pair]
    gate_rows, up_rows = unpack(both[20:22] + both[10:12] + both[0:10], both[12:20])
    return gate_rows, up_rows, hid


def solution(mesh):
    split = Mesh(mesh.devices.reshape(NX, NZ, NC, 2, 4), ROW + COL)
    return jax.shard_map(
        body,
        mesh=split,
        in_specs=(P(None, None, ROW, None, COL), P(None, None, COL)),
        out_specs=(P(None, ROW, COL), P(None, ROW, COL), P(None, COL, ROW)),
        check_vma=False,
    )
```

```python
import jax
import jax.numpy as jnp
from jax import lax
from jax.experimental import pallas as pl
from jax.experimental.pallas import tpu as pltpu
from jax.sharding import Mesh
from jax.sharding import PartitionSpec as P

ROW = ("xlo", "z", "core")
COL = ("xhi", "y")
NX, NZ, NC = 2, 8, 2
EARLY = (3, 5)
LATE = (2, 6, 1, 7)
FLIPPED = (0,) + LATE
PIECES = tuple((a, s) for s in EARLY for a in (0, 1)) + ((0, 4), (1, 4)) + tuple((1, s) for s in FLIPPED) + tuple((0, s) for s in LATE) + ((0, 0),)
FIRST = PIECES[:4] + PIECES[6:11]
SECOND = PIECES[4:6] + PIECES[11:]
PIECE = (56, 512)


def row_index(x, z, c):
    return (x * NZ + z) * NC + c


def hop(a, s, b):
    return [
        (row_index(x, z, c), row_index(x ^ a, (z + s) % NZ, c ^ b))
        for x in range(NX)
        for z in range(NZ)
        for c in range(NC)
    ]


def vmem(*shape, dtype=jnp.bfloat16):
    return pltpu.VMEM(shape, dtype)


def hbm(*shape, dtype=jnp.bfloat16):
    return pltpu.HBM(shape, dtype)


def inside(x):
    return pltpu.with_memory_space_constraint(x, pltpu.VMEM)


def outside(x):
    return pltpu.with_memory_space_constraint(x, pltpu.HBM)


WHOLE = pl.BlockSpec(memory_space=pltpu.VMEM)
ANYWHERE = pl.BlockSpec(memory_space=pl.ANY)
INHBM = pl.BlockSpec(memory_space=pltpu.HBM)


def params(mib):
    return pltpu.CompilerParams(vmem_limit_bytes=mib << 20)


def selection(pieces):
    x, z, c = lax.axis_index("xlo"), lax.axis_index("z"), lax.axis_index("core")
    row = lax.broadcasted_iota(jnp.int32, (16 * len(pieces), 256), 0)
    column = lax.broadcasted_iota(jnp.int32, (16 * len(pieces), 256), 1)
    j, b, n = row & 7, (row >> 3) & 1, row >> 4
    flip, step = jnp.zeros_like(n), jnp.zeros_like(n)
    for i, (a, s) in enumerate(pieces):
        flip = jnp.where(n == i, a, flip)
        step = jnp.where(n == i, s, step)
    block = ((flip ^ x) << 4) + (((z + step) & 7) << 1) + (b ^ c)
    return (column == (j << 5) + block).astype(jnp.bfloat16)


def pack_first_kernel(w_hbm, *refs):
    outs, w, sems = refs[:3], refs[3], refs[4]
    copies = [pltpu.make_async_copy(w_hbm.at[pl.ds(8 * g, 8)], w.at[pl.ds(8 * g, 8)], sems.at[g]) for g in range(7)]
    for copy in copies:
        copy.start()
    pick = selection(FIRST)
    for g in range(7):
        copies[g].wait()
        rows = w[8 * g : 8 * g + 8].reshape(256, 512)
        moved = jnp.dot(pick, rows, preferred_element_type=jnp.float32).astype(jnp.bfloat16)
        moved = moved.reshape(9, 2, 8, 512)
        for out, first, count in zip(outs, (0, 2, 4), (2, 2, 5)):
            out[:, :, 8 * g : 8 * g + 8, :] = moved[first : first + count]


def pack_first(w):
    return pl.pallas_call(
        pack_first_kernel,
        out_shape=[vmem(2, 2, *PIECE)] * 2 + [vmem(5, 2, *PIECE), vmem(56, 32, 512)],
        in_specs=[INHBM],
        out_specs=[WHOLE] * 4,
        scratch_shapes=[pltpu.SemaphoreType.DMA((7,))],
        compiler_params=params(4),
        name="pack_first",
    )(outside(w))


def pack_second_kernel(w, probes_hbm, *refs):
    outs, parts, (held, probes, proj, sems, out_sems, part_sems) = refs[:8], refs[8:12], refs[12:]
    y = lax.axis_index("y")
    first = pltpu.make_async_copy(probes_hbm, probes, sems.at[0])
    first.start()
    pick = selection(SECOND)
    dims = (((1,), (1,)), ((), ()))
    sent = []

    def ship(half, begin, count):
        rows = pl.ds(begin, count)
        pairs = [(held.at[i, :, rows], outs[i].at[:, rows]) for i in range(2)]
        pairs.append((held.at[2, :, rows], outs[6].at[:, rows]))
        for i, (source, target) in enumerate(pairs):
            sent.append(pltpu.make_async_copy(source, target, out_sems.at[3 * half + i]))
            sent[-1].start()

    for layer in range(2):
        part = w[28 * layer : 28 * layer + 28].reshape(896, 512)
        if layer == 0:
            first.wait()
        product = lax.dot_general(probes[layer], part, dims, preferred_element_type=jnp.float32)
        proj[layer] = product.reshape(8, 16, 896)
        for s in range(1, 4):
            for h in range(2):
                n = len(sent)
                source = proj.at[layer, 4 * h + ((y + s) & 3)]
                sent.append(pltpu.make_async_copy(source, parts[s].at[h, layer], part_sems.at[n]))
                sent[-1].start()
        for h in range(2):
            parts[0][h, layer] = proj[layer, 4 * h + y]
    for g in range(7):
        rows = w[8 * g : 8 * g + 8].reshape(256, 512)
        moved = jnp.dot(pick, rows, preferred_element_type=jnp.float32).astype(jnp.bfloat16)
        moved = moved.reshape(7, 2, 8, 512)
        here = slice(8 * g, 8 * g + 8)
        held[:2, :, here, :] = moved[:2]
        held[2, :, here, :] = moved[6]
        for i in range(4):
            outs[2 + i][0, 0, here, :] = moved[2 + i, 0]
            outs[7][i, here, :] = moved[2 + i, 1]
        if g == 3:
            ship(0, 0, 32)
    ship(1, 32, 24)
    for copy in sent:
        copy.wait()


def pack_second(w, probes):
    return pl.pallas_call(
        pack_second_kernel,
        out_shape=[hbm(2, *PIECE)] * 2
        + [vmem(2, 2, *PIECE)] * 4
        + [hbm(2, *PIECE), vmem(4, *PIECE)]
        + [vmem(2, 2, 16, 896, dtype=jnp.float32)]
        + [hbm(2, 2, 16, 896, dtype=jnp.float32)] * 3,
        in_specs=[WHOLE, INHBM],
        out_specs=[INHBM] * 2 + [WHOLE] * 4 + [INHBM] + [WHOLE] * 2 + [INHBM] * 3,
        scratch_shapes=[
            pltpu.VMEM((3, 2, 56, 512), jnp.bfloat16),
            pltpu.VMEM((2, 128, 512), jnp.bfloat16),
            pltpu.VMEM((2, 8, 16, 896), jnp.float32),
            pltpu.SemaphoreType.DMA((1,)),
            pltpu.SemaphoreType.DMA((6,)),
            pltpu.SemaphoreType.DMA((12,)),
        ],
        compiler_params=params(8),
        name="pack_second",
    )(inside(w), outside(probes))


def join_kernel(crossed, crossed_swapped, got, *refs):
    outs, near = refs[4:8], refs[8]
    for n, out in enumerate(outs):
        out[0, 1] = got[n]
        out[1, 0] = crossed[1 + n, 0]
        out[1, 1] = crossed_swapped[1 + n, 1]
    near[0] = crossed[0, 0]
    near[1] = crossed_swapped[0, 1]


def join(crossed, crossed_swapped, got, straight):
    return pl.pallas_call(
        join_kernel,
        out_shape=[vmem(2, 2, *PIECE)] * 4 + [vmem(2, *PIECE)],
        in_specs=[WHOLE] * 7,
        out_specs=[WHOLE] * 5,
        input_output_aliases={3: 0, 4: 1, 5: 2, 6: 3},
        compiler_params=params(1),
        name="join",
    )(*map(inside, (crossed, crossed_swapped, got, *straight)))


def gather_kernel(*refs):
    pieces, out, sems = refs[:2], refs[2], refs[3]
    copies = [pltpu.make_async_copy(piece.at[1], out.at[n], sems.at[n]) for n, piece in enumerate(pieces)]
    for copy in copies:
        copy.start()
    for copy in copies:
        copy.wait()


def gather(pieces):
    return pl.pallas_call(
        gather_kernel,
        out_shape=vmem(2, 2, *PIECE),
        in_specs=[ANYWHERE] * 2,
        out_specs=WHOLE,
        scratch_shapes=[pltpu.SemaphoreType.DMA((2,))],
        compiler_params=params(1),
        name="gather",
    )(*pieces)


def unpack_kernel(*refs):
    early, late, (gate_hbm, up_hbm, held, rows_out, out_sems) = refs[:13], refs[13:17], refs[17:]
    x, z, c = lax.axis_index("xlo"), lax.axis_index("z"), lax.axis_index("core")
    local, near, z3, z5, d04, d14, post = early[0:2], early[2], early[3:5], early[5:7], early[7:9], early[9:11], early[11:13]
    pieces = []
    for b in range(2):
        pieces += [(local[b].at[b], 0, 0, b), (near.at[b], 1, 0, b)]
        pieces += [(z3[b].at[0, b], 0, 3, b), (post[b].at[0, b], 1, 3, b)]
        pieces += [(z5[b].at[0, b], 0, 5, b), (post[b].at[1, b], 1, 5, b)]
        pieces += [(d04[b].at[b], 0, 4, b), (d14[b].at[b], 1, 4, b)]

    def place(a, s, b):
        return (a ^ x) * 4 + (((z - s) & 7) >> 1), (z - s) & 1, b ^ c

    out = lax.broadcasted_iota(jnp.int32, (224, 224), 0)
    inn = lax.broadcasted_iota(jnp.int32, (224, 224), 1)
    source = jnp.zeros((224, 224), jnp.int32)
    for q in range(4):
        for layer in range(2):
            for g in range(2):
                first = (layer * 2 + g) * 56 + q * 14
                here = (out >= first) & (out < first + 14)
                source = jnp.where(here, q * 56 + layer * 28 + g + 2 * (out - first), source)
    pick = (inn == source).astype(jnp.bfloat16)
    for i, s in enumerate(LATE):
        for a in range(2):
            for b in range(2):
                held[place(a, s, b)] = late[i][a, b]
    for source, a, s, b in pieces:
        held[place(a, s, b)] = source[...]
    copies = []
    for n in range(8):
        rows = held[n].reshape(224, 512)
        moved = jnp.dot(pick, rows, preferred_element_type=jnp.float32).astype(jnp.bfloat16)
        for layer in range(2):
            for g in range(2):
                first = (layer * 2 + g) * 56
                rows_out[n, g, layer] = moved[first : first + 56]
        for g, target in enumerate((gate_hbm, up_hbm)):
            copy = pltpu.make_async_copy(rows_out.at[n, g], target.at[:, pl.ds(56 * n, 56)], out_sems.at[2 * n + g])
            copy.start()
            copies.append(copy)
    for copy in copies:
        copy.wait()


def unpack(early, late):
    return pl.pallas_call(
        unpack_kernel,
        out_shape=[hbm(2, 448, 512)] * 2,
        in_specs=[WHOLE] * 17,
        out_specs=[INHBM] * 2,
        scratch_shapes=[
            pltpu.VMEM((8, 2, 2, 56, 512), jnp.bfloat16),
            pltpu.VMEM((8, 2, 2, 56, 512), jnp.bfloat16),
            pltpu.SemaphoreType.DMA((16,)),
        ],
        compiler_params=params(10),
        name="unpack",
    )(*map(inside, early), *map(inside, late))


def halve_kernel(p0, p1, p2, p3, keep, give):
    h = lax.axis_index("xhi")
    keep[...] = (p0[h] + p1[h]) + (p2[h] + p3[h])
    give[...] = (p0[1 - h] + p1[1 - h]) + (p2[1 - h] + p3[1 - h])


def halve(parts):
    return pl.pallas_call(
        halve_kernel,
        out_shape=[vmem(2, 16, 896, dtype=jnp.float32)] * 2,
        in_specs=[WHOLE] * 4,
        out_specs=[WHOLE] * 2,
        compiler_params=params(8),
        name="halve",
    )(inside(parts[0]), *parts[1:])


def gated_kernel(keep, came, out_ref):
    total = (keep[...] + came[...]).reshape(32, 896)
    up = pltpu.roll(total, 896 - 32, 1)
    turned = (total / (1.0 + jnp.exp(-total)) * up).T
    quads = []
    for q in range(4):
        blocks = [turned[64 * i : 64 * i + 32] if i < 14 else jnp.zeros((32, 32), jnp.float32) for i in range(4 * q, 4 * q + 4)]
        quads.append(jnp.concatenate(blocks, axis=1))
    rows = jnp.concatenate(quads, axis=0).astype(jnp.bfloat16)
    to = lax.broadcasted_iota(jnp.int32, (128, 128), 0)
    of = lax.broadcasted_iota(jnp.int32, (128, 128), 1)
    pick = (of == ((to & 3) << 5) + (to >> 2)).astype(jnp.bfloat16)
    out_ref[...] = jnp.dot(pick, rows, preferred_element_type=jnp.float32).astype(jnp.bfloat16)


def gated(keep, came):
    return pl.pallas_call(
        gated_kernel,
        out_shape=jax.ShapeDtypeStruct((128, 128), jnp.bfloat16),
        in_specs=[WHOLE] * 2,
        out_specs=WHOLE,
        compiler_params=params(8),
        name="gated",
    )(inside(keep), inside(came))


def final_kernel(came, out_ref):
    turned = came[...].astype(jnp.float32).T.astype(jnp.bfloat16)
    of = lax.broadcasted_iota(jnp.int32, (128, 512), 0)
    to = lax.broadcasted_iota(jnp.int32, (128, 512), 1)
    pick = (to == (of >> 2) * 14 + ((of & 3) << 2)).astype(jnp.bfloat16)
    spread = jnp.dot(turned, pick, preferred_element_type=jnp.float32)
    total = spread[:32]
    for i in range(1, 4):
        total += pltpu.roll(spread[32 * i : 32 * i + 32], i, 1)
    out_ref[...] = total[:, :448].astype(jnp.bfloat16).reshape(2, 16, 448)


def final(came):
    return pl.pallas_call(
        final_kernel,
        out_shape=jax.ShapeDtypeStruct((2, 16, 448), jnp.bfloat16),
        in_specs=[WHOLE],
        out_specs=WHOLE,
        compiler_params=params(8),
        name="final",
    )(came)


def send(piece, a, s, b):
    return lax.ppermute(piece, ROW, hop(a, s, b))


def side(piece, h, y):
    pairs = [(p * 4 + q, (p ^ h) * 4 + (q + y) % 4) for p in range(2) for q in range(4)]
    return lax.ppermute(piece, COL, pairs)


def body(joined, probes):
    w = joined.reshape(2, 32, 28, 512).transpose(0, 2, 1, 3).reshape(56, 32, 512)
    *outs, w = pack_first(w)
    rest = pack_second(w, probes)
    outs, give_core, parts = [*outs[:2], *rest[:2], outs[2], *rest[2:7]], rest[7], rest[8:]
    early = [send(piece, 0, s, 0) for s, piece in zip(EARLY, outs)]
    across = [send(piece, a, 4, 0) for a, piece in zip((0, 1), outs[2:4])]
    crossed = send(outs[4], 1, 0, 0)
    parts = [parts[0]] + [side(parts[s], 0, s) for s in range(1, 4)]
    keep, give = halve(parts)
    came = side(give, 1, 0)
    got_core = send(give_core, 0, 0, 1)
    crossed_swapped = send(crossed, 0, 0, 1)
    *joins, near = join(crossed, crossed_swapped, got_core, outs[5:9])
    late = [send(piece, 0, s, 0) for s, piece in zip(LATE, joins)]
    post = gather(early)
    post = send(post, 1, 0, 0)
    mine = early + across + [post, outs[9]]
    other = [send(piece, 0, 0, 1) for piece in mine]
    hid = gated(keep, came).reshape(32, 4, 128)
    hid = lax.all_to_all(hid, ROW, 0, 0, tiled=True)
    hid = final(hid.reshape(128, 128))
    both = [piece for pair in zip(mine, other) for piece in pair]
    gate_rows, up_rows = unpack(both[10:12] + [near] + both[:10], late)
    return gate_rows, up_rows, hid


def solution(mesh):
    split = Mesh(mesh.devices.reshape(NX, NZ, NC, 2, 4), ROW + COL)
    return jax.shard_map(
        body,
        mesh=split,
        in_specs=(P(None, None, ROW, None, COL), P(None, None, COL)),
        out_specs=(P(None, ROW, COL), P(None, ROW, COL), P(None, COL, ROW)),
        check_vma=False,
    )
```
